1024 devices in a mesh: img: 64 (over x, z), tile: 16 (over y, core).
Axes of the slice: x: 8, y: 8, z: 8, core: 2. Of those that a mesh axis runs over, the one named last changes fastest.
Arguments:
- query: bfloat16 [64, 2048, 1280], P('img', 'tile'), may hold values from -6 to 6
- keys: bfloat16 [64, 2048, 1280], P('img', 'tile'), may hold values from -6 to 6
- values: bfloat16 [64, 2048, 1280], P('img', 'tile'), may hold values from -6 to 6
- out_weight: bfloat16 [1280, 1280], P('tile'), may hold values from -0.15625 to 0.15625
- hidden: bfloat16 [64, 2048, 1280], P('img', 'tile'), may hold values from -36 to 36
- gain: float32 [1280], replicated, may hold values from 0.5 to 1.5
- seq_grad: bfloat16 [64, 2048, 5120], P('img', 'tile'), may hold values from -6 to 6
- splice_at: int32 [64, 512], P('img', 'tile'), may hold values from 0 to 2047, as said below
- merged_count: int32 [64], P('img'), may hold values from 64 to 512
Outputs:
- query_grad: bfloat16 [64, 2048, 1280], P('img', 'tile')
- key_grad: bfloat16 [64, 2048, 1280], P('img', 'tile')
- value_grad: bfloat16 [64, 2048, 1280], P('img', 'tile')
- gain_grad: float32 [1280], replicated
The draws below stay inside these ranges and needn't reach their ends.
Inputs may be any that keep to these rules, and one draw needn't show every extreme that they name: `splice_at`: within one image the positions are distinct. The merged rows of one device (aligned blocks of 32 rows) place at most 4 rows in any one block of 128 positions of the sequence.
All inputs are finite; a program needn't handle non-finite values.
Results may differ from the reference program's by a relative error of at most 0.009.
Values may be sent and summed in bfloat16 or wider, within the bound.
A program may use at most 32 MiB of HBM per device.

```python
import jax
import jax.numpy as jnp
from jax import lax

HEADS = 16
HEAD = 80
D = 1280
CTX_DEV = 128
IMAGES = 64
PATCHES = 2048
MERGED = 512
MERGED_DEV = 32
CAP = 4
SEQ_LEN = 2048


def drawn_pair(key):
    first = jax.random.fold_in(key, 11)
    second = jax.random.fold_in(key, 12)
    query_base = 1.5 * jax.random.truncated_normal(first, -4.0, 4.0, (IMAGES, PATCHES, D), jnp.float32)
    keys_base = 1.5 * jax.random.truncated_normal(second, -4.0, 4.0, (IMAGES, PATCHES, D), jnp.float32)
    return (query_base, keys_base)


def draw_query(key, part):
    return drawn_pair(key)[0].astype(jnp.bfloat16)


def draw_keys(key, part):
    return drawn_pair(key)[1].astype(jnp.bfloat16)


def draw_hidden(key, part):
    base_key = jax.random.fold_in(key, 21)
    row_key = jax.random.fold_in(key, 22)
    column_key = jax.random.fold_in(key, 23)
    base = jax.random.truncated_normal(base_key, -4.0, 4.0, (IMAGES, PATCHES, D), jnp.float32)
    row_scale = jnp.exp(jax.random.uniform(row_key, (IMAGES, PATCHES, 1), jnp.float32, jnp.log(0.3), jnp.log(3.0)))
    column_scale = jnp.exp(jax.random.uniform(column_key, (D,), jnp.float32, jnp.log(0.5), jnp.log(2.0)))
    return (base * row_scale * column_scale).astype(jnp.bfloat16)


def draw_splice_at(key, part):
    groups = MERGED // MERGED_DEV
    slot_total = groups * CAP
    full_key = jax.random.fold_in(key, 31)
    order_key = jax.random.fold_in(key, 32)
    shuffle_key = jax.random.fold_in(key, 33)
    place_key = jax.random.fold_in(key, 34)
    full_span = jax.random.randint(full_key, (IMAGES, 1, 1), 0, groups)
    order_keys = jax.random.split(order_key, IMAGES * groups)
    ranking = jax.vmap(lambda each: jax.random.permutation(each, slot_total))(order_keys).reshape(IMAGES, groups, slot_total)
    slot_range = jnp.arange(slot_total, dtype=jnp.int32)
    priority = ranking + jnp.where(slot_range // CAP == full_span, slot_total, 0)
    chosen = jnp.argsort(-priority, axis=-1, stable=True)[..., :MERGED_DEV]
    shuffle_keys = jax.random.split(shuffle_key, IMAGES * groups)
    shuffled = jax.vmap(lambda each: jax.random.permutation(each, MERGED_DEV))(shuffle_keys).reshape(IMAGES, groups, MERGED_DEV)
    chosen = jnp.take_along_axis(chosen, shuffled, axis=-1)
    spans = chosen // CAP
    within = chosen % CAP
    place_keys = jax.random.split(place_key, IMAGES * groups)
    places = jax.vmap(lambda each: jax.random.permutation(each, CTX_DEV))(place_keys).reshape(IMAGES, groups * CTX_DEV)
    sources = jnp.arange(groups, dtype=jnp.int32)[None, :, None]
    lookup = (spans * CTX_DEV + sources * CAP + within).reshape(IMAGES, MERGED)
    inside = jnp.take_along_axis(places, lookup, axis=1)
    return (spans.reshape(IMAGES, MERGED) * CTX_DEV + inside).astype(jnp.int32)


def place_ends(values, stream_key, least, high):
    index_at = [jax.random.randint(jax.random.fold_in(stream_key, axis), (), 0, length) for axis, length in enumerate(values.shape)]
    longest = values.shape.index(max(values.shape))
    beside = index_at[:longest] + [(index_at[longest] + 1) % values.shape[longest]] + index_at[longest + 1:]
    return values.at[tuple(index_at)].set(least).at[tuple(beside)].set(high)


def levels(own_key, shape, cuts, low, high):
    level = 1.0
    for axis_at, parts in cuts:
        steps = jax.random.uniform(jax.random.fold_in(jax.random.fold_in(own_key, 6), axis_at), (parts,), jnp.float32, low / len(cuts), high / len(cuts))
        level = level * jnp.repeat(jnp.exp(steps), shape[axis_at] // parts).reshape((-1,) + (1,) * (len(shape) - 1 - axis_at))
    return level


def bell_draw(own_key, shape, deviation, most, shards=(), kind=jnp.bfloat16):
    result = deviation * jax.random.normal(own_key, shape, jnp.float32)
    if shards:
        result = result * levels(own_key, shape, shards, -0.22, 0.18)
    return jnp.clip(result, -most, most).astype(kind)


def setup_inputs(seed: int = 0) -> dict:
    key_list = jax.random.split(jax.random.key(seed), 10)
    query = draw_query(jax.random.fold_in(key_list[9], 71), 0)
    keys = draw_keys(jax.random.fold_in(key_list[9], 71), 0)
    values = bell_draw(key_list[2], (IMAGES, PATCHES, D), 1.0, 6.0, ((0, 64), (1, 16)))
    out_weight = bell_draw(key_list[3], (D, D), D ** -0.5, 0.15625, ((0, 16),))
    hidden = draw_hidden(jax.random.fold_in(key_list[9], 71), 0)
    gain = jnp.clip(1.0 + 0.1 * jax.random.normal(key_list[5], (D,), jnp.float32), 0.5, 1.5)
    seq_grad = bell_draw(key_list[6], (IMAGES, SEQ_LEN, 4 * D), 1.0, 6.0, ((0, 64), (1, 16)))
    splice_at = draw_splice_at(jax.random.fold_in(key_list[9], 71), 0)
    merged_count = place_ends(jax.random.randint(key_list[8], (IMAGES,), MERGED // 8, MERGED + 1), jax.random.fold_in(key_list[8], 1), MERGED // 8, MERGED).astype(jnp.int32)
    return {"query": query, "keys": keys, "values": values, "out_weight": out_weight, "hidden": hidden, "gain": gain, "seq_grad": seq_grad, "splice_at": splice_at, "merged_count": merged_count}


norm_eps = 1e-06

def head_backward(packed, key_live):
    head_query, head_keys, head_values, head_grad = packed
    factor = HEAD ** (-0.5)
    scores = jnp.dot(head_query, head_keys.T, preferred_element_type=jnp.float32) * factor
    scores = jnp.where(key_live[None, :], scores, -1e+30)
    largest = lax.optimization_barrier(jnp.max(scores, axis=-1, keepdims=True))
    expons = jnp.exp(scores - largest)
    probs = expons / lax.optimization_barrier(jnp.sum(expons, axis=-1, keepdims=True))
    low_probs = probs.astype(jnp.bfloat16)
    value_part = jnp.dot(low_probs.T, head_grad, preferred_element_type=jnp.float32).astype(jnp.bfloat16)
    dprobs = jnp.dot(head_grad, head_values.T, preferred_element_type=jnp.float32)
    spread = lax.optimization_barrier(jnp.sum(probs * dprobs, axis=-1, keepdims=True))
    dscores = (probs * (dprobs - spread)).astype(jnp.bfloat16)
    query_part = (jnp.dot(dscores, head_keys, preferred_element_type=jnp.float32) * factor).astype(jnp.bfloat16)
    key_part = (jnp.dot(dscores.T, head_query, preferred_element_type=jnp.float32) * factor).astype(jnp.bfloat16)
    return (query_part, key_part, value_part)

def split_heads(matrix):
    return matrix.reshape(PATCHES, HEADS, HEAD).transpose(1, 0, 2)

def join_heads(stacked):
    return stacked.transpose(1, 0, 2).reshape(PATCHES, D)

def reference(query, keys, values, out_weight, hidden, gain, seq_grad, splice_at, merged_count):

    def image_grads(packed):
        query_img, keys_img, values_img, hidden_img, seq_img, spots_img, count_img = packed
        picked = jnp.take(seq_img, spots_img, axis=0)
        live_rows = jnp.arange(MERGED) < count_img
        merged = jnp.where(live_rows[:, None], picked, jnp.zeros((), picked.dtype))
        upstream = merged.reshape(PATCHES, D).astype(jnp.float32)
        values32 = hidden_img.astype(jnp.float32)
        inverse = lax.rsqrt(lax.optimization_barrier(jnp.mean(values32 * values32, axis=-1, keepdims=True)) + norm_eps)
        normed = values32 * inverse
        gain_part = lax.optimization_barrier(jnp.sum(upstream * normed, axis=0))
        scaled = gain * upstream
        attn_grad = (inverse * (scaled - normed * lax.optimization_barrier(jnp.mean(scaled * normed, axis=-1, keepdims=True)))).astype(jnp.bfloat16)
        core_grad = jnp.dot(attn_grad, out_weight.T, preferred_element_type=jnp.float32).astype(jnp.bfloat16)
        key_live = jnp.arange(PATCHES) < 4 * count_img
        stacked = lax.map(lambda item: head_backward(item, key_live), (split_heads(query_img), split_heads(keys_img), split_heads(values_img), split_heads(core_grad)))
        return (join_heads(stacked[0]), join_heads(stacked[1]), join_heads(stacked[2]), gain_part)
    query_grad, key_grad, value_grad, gain_parts = lax.map(image_grads, (query, keys, values, hidden, seq_grad, splice_at, merged_count))
    gain_grad = lax.optimization_barrier(jnp.sum(gain_parts, axis=0))
    return (query_grad, key_grad, value_grad, gain_grad)
```

```python
import math

import jax
import jax.numpy as jnp
from jax import lax
from jax.experimental import pallas as pl
from jax.experimental.pallas import tpu as pltpu
from jax.sharding import PartitionSpec as P

MESH = pl.DeviceIdType.MESH
F32 = jnp.float32
BF16 = jnp.bfloat16

NORM_EPS = 1e-06
HEAD = 80
D = 1280
T = 16
ROWS = 128
PATCHES = 2048
HALF = 640
QB = 256
FACTOR = HEAD ** (-0.5)
REQ, W1, W2, W3, ROW, Q, K, V, G, DQ, DK, DV, GA, GB, GC = range(15)


def dot(a, b, ca, cb):
    return lax.dot_general(a, b, (((ca,), (cb,)), ((), ())), preferred_element_type=F32)


def kernel(
    pos_ref, count_ref, q_ref, k_ref, v_ref, w_ref, h_ref, gain_ref, seq_ref,
    oq_ref, ok_ref, ov_ref, og_ref,
    qs, ks, vs, gs, qt, kt, vt, gt, wall, reqs, reqr, reqt, rsend, rrecv,
    probs, dv, dk, dqb, dkb, dvb, bq, bk, bv,
    g1s, g1, g2s, g2, g3s, g3, ssem, rsem,
):
    img = lax.axis_index("img")
    tile = lax.axis_index("tile")
    x, z = img // 8, img % 8
    y, c = tile // 2, tile % 2
    u = x * (1 - c) + z * c
    sigma = u % 4
    me80 = pl.multiple_of(tile * HEAD, 16)
    me128 = pl.multiple_of(tile * ROWS, ROWS)

    def peer(delta):
        return (tile + delta) % T

    def along(d):
        return ((x + (1 - c) * d) % 8) * 8 + (z + c * d) % 8

    def on_x(d):
        return ((x + d) % 8) * 8 + z

    def on_z(d):
        return x * 8 + (z + d) % 8

    def link(src, dst, kind, to_img, to_tile):
        return pltpu.make_async_remote_copy(
            src_ref=src,
            dst_ref=dst,
            send_sem=ssem.at[kind],
            recv_sem=rsem.at[kind],
            device_id=(to_img, to_tile),
            device_id_type=MESH,
        )

    def arrived(ref, kind):
        link(ref, ref, kind, img, peer(1)).wait_recv()

    def sent(ref, kind):
        link(ref, ref, kind, img, peer(1)).wait_send()

    def to_tiles(fn):
        def step(delta, carry):
            fn(peer(delta))
            return carry

        lax.fori_loop(1, T, step, 0)

    barrier = pltpu.get_barrier_semaphore()

    def hello(to_img, to_tile):
        pl.semaphore_signal(barrier, inc=1, device_id=(to_img, to_tile), device_id_type=MESH)

    def hello_plane(delta, carry):
        hello(on_x(delta), tile)
        hello(on_z(delta), tile)
        return carry

    to_tiles(lambda t: hello(img, t))
    lax.fori_loop(1, 8, hello_plane, 0)

    count = count_ref[0]
    lane = lax.broadcasted_iota(jnp.int32, (8, 128), 1)
    span = lax.broadcasted_iota(jnp.int32, (8, 128), 0) * 4 + lane // 32
    slot = lane % 4
    part = (lane % 32) // 4
    seen = jnp.zeros((8, 128), jnp.int32)
    want = jnp.full((8, 128), -1, jnp.int32)
    whose = jnp.full((8, 128), -1, jnp.int32)
    for r in range(32):
        at = pos_ref[0, r]
        live = jnp.where(tile * 32 + r < count, at // 128, -1)
        take = (span == live) & (seen == slot)
        want = jnp.where(take, at % 128, want)
        whose = jnp.where(take, r, whose)
        seen = seen + jnp.where(span == live, 1, 0)
    for o in range(4):
        reqs[o] = want[o : o + 1]

    for src, mid, dst in ((q_ref, qs, qt), (k_ref, ks, kt), (v_ref, vs, vt)):
        for b in range(10):
            mid[b * 128 : (b + 1) * 128, :] = src[:, b * 128 : (b + 1) * 128].T
        dst[0:HEAD, pl.ds(me128, ROWS)] = mid[pl.ds(me80, HEAD), :]
    row0 = lax.broadcasted_iota(jnp.int32, (48, PATCHES), 0) == 0
    key_at = lax.broadcasted_iota(jnp.int32, (48, PATCHES), 1)
    qt[HEAD:128, :] = jnp.where(row0, 1.0, 0.0).astype(BF16)
    kt[HEAD:128, :] = jnp.where(row0 & (key_at >= 4 * count), -1e30, 0.0).astype(BF16)
    vt[HEAD:128, :] = jnp.zeros((48, PATCHES), BF16)
    gt[HEAD:128, :] = jnp.zeros((48, PATCHES), BF16)
    dv[...] = jnp.zeros_like(dv)
    dk[...] = jnp.zeros_like(dk)
    reqr[pl.ds(tile, 1)] = reqs[pl.ds(tile // 4, 1)]
    w_rows = pl.ds(pl.multiple_of((sigma // 2) * 32, 32), 48)
    w_cols = pl.ds(pl.multiple_of((sigma % 2) * HALF, 128), HALF)
    wall[c, sigma, y] = w_ref[w_rows, w_cols]

    pl.semaphore_wait(barrier, T - 1 + 14)

    to_tiles(lambda t: link(reqs.at[t // 4], reqr.at[tile], REQ, img, t).start())

    def send_w1(delta, carry):
        link(w_ref.at[w_rows, w_cols], wall.at[c, sigma, y], W1, img, (tile + 2 * delta) % T).start()
        return carry

    lax.fori_loop(1, 8, send_w1, 0)

    arrived(reqr.at[0 : T - 1], REQ)
    asked = reqr[...].reshape(T, 128).astype(F32)
    reqt[...] = jnp.concatenate([asked, jnp.full((112, 128), -1.0, F32)], axis=0).T
    mine = reqt[pl.ds(pl.multiple_of((tile % 4) * 32, 32), 32), :].astype(jnp.int32)
    wide = lax.broadcasted_iota(jnp.int32, (32, 128), 1)
    row_part = lax.broadcasted_iota(jnp.int32, (32, 128), 0) // 4
    for d in range(0, T, 4):
        hits = [jnp.broadcast_to(mine[:, e : e + 1], (32, 128)) == wide for e in range(d, d + 4)]
        rows = jnp.zeros((128, HALF), F32)
        for s in range(8):
            pick = jnp.concatenate(
                [jnp.where(hit & (row_part == s), 1.0, 0.0) for hit in hits], axis=0
            ).astype(BF16)
            rows = rows + dot(pick, seq_ref[:, s * HALF : (s + 1) * HALF], 1, 0)
        rsend[d : d + 4] = rows.astype(BF16).reshape(4, 32, HALF)
    rrecv[pl.ds(tile, 1)] = rsend[pl.ds(tile, 1)]
    to_tiles(lambda t: link(rsend.at[t], rrecv.at[tile], ROW, img, t).start())

    def block_of(ref, t):
        return ref.at[pl.ds(pl.multiple_of(t * HEAD, 16), HEAD), :]

    def head_rows(ref):
        return ref.at[0:HEAD, pl.ds(me128, ROWS)]

    to_tiles(lambda t: link(block_of(qs, t), head_rows(qt), Q, img, t).start())
    to_tiles(lambda t: link(block_of(ks, t), head_rows(kt), K, img, t).start())
    to_tiles(lambda t: link(block_of(vs, t), head_rows(vt), V, img, t).start())

    own = wall.at[c, sigma]
    lower, upper = wall.at[c, sigma, 0:4], wall.at[c, sigma, 4:8]
    other = tile + 1 - 2 * c
    arrived(wall.at[0, 0, 0:7], W1)
    link(own, own, W2, along(1), tile).start()
    link(own, own, W2, along(7), tile).start()
    link(lower, lower, W2, along(2), tile).start()
    link(upper, upper, W2, along(6), tile).start()
    link(own, own, W3, img, other).start()
    arrived(wall.at[0, 0:3], W2)
    for i in range(1, 4):
        more = wall.at[c, (sigma + i) % 4]
        link(more, more, W3, img, other).start()

    hidden = h_ref[...].astype(F32)
    inverse = lax.rsqrt(jnp.mean(hidden * hidden, axis=1, keepdims=True) + NORM_EPS)
    normed = hidden * inverse
    wide_rows = lax.broadcasted_iota(jnp.int32, (ROWS, 128), 0)
    lane_part = (lax.broadcasted_iota(jnp.int32, (ROWS, 128), 1) % 32) // 4
    arrived(rrecv.at[0 : T - 1], ROW)
    halves = []
    for h in range(2):
        total = jnp.zeros((ROWS, HALF), F32)
        for o in range(4):
            owner = jnp.broadcast_to(whose[o : o + 1], (ROWS, 128))
            pick = (owner == wide_rows // 4) & (lane_part == 2 * (wide_rows % 4) + h)
            total = total + dot(
                jnp.where(pick, 1.0, 0.0).astype(BF16),
                rrecv[4 * o : 4 * o + 4].reshape(128, HALF),
                1,
                0,
            )
        halves.append(total)
    upstream = jnp.concatenate(halves, axis=1)
    both = upstream * normed
    part_sum = jnp.sum(both, axis=0, keepdims=True)
    gain = gain_ref[...]
    mean = jnp.mean(gain * both, axis=1, keepdims=True)
    attn = (inverse * (gain * upstream - normed * mean)).astype(BF16)
    g1s[...] = part_sum
    g1[pl.ds(tile, 1)] = part_sum.reshape(1, 1, D)

    arrived(wall.at[0], W3)
    for c2 in range(2):
        for ch in range(2):
            acc = jnp.zeros((384, ROWS), F32)
            for dh in range(2):
                acc = acc + dot(
                    wall[c2, ch * 2 + dh].reshape(384, HALF), attn[:, dh * HALF : (dh + 1) * HALF], 1, 1
                )
            acc = acc.astype(BF16)
            for y2 in range(8):
                base = (2 * y2 + c2) * HEAD
                if ch == 0:
                    gs[base : base + 48, :] = acc[48 * y2 : 48 * y2 + 48]
                else:
                    gs[base + 48 : base + 80, :] = acc[48 * y2 + 16 : 48 * y2 + 48]
    gt[0:HEAD, pl.ds(me128, ROWS)] = gs[pl.ds(me80, HEAD), :]
    to_tiles(lambda t: link(g1s, g1.at[tile], GA, img, t).start())
    to_tiles(lambda t: link(block_of(gs, t), head_rows(gt), G, img, t).start())

    arrived(qt.at[0:HEAD, 0 : PATCHES - ROWS], Q)
    arrived(kt.at[0:HEAD, 0 : PATCHES - ROWS], K)
    rate = FACTOR * math.log2(math.e)

    def soften(j, carry):
        at = pl.ds(pl.multiple_of(j * QB, QB), QB)
        scores = dot(qt[:, at].T, kt[...], 1, 0)
        largest = jnp.max(scores, axis=1, keepdims=True)
        expons = jnp.exp2((scores - largest) * rate)
        probs[at, :] = (expons * (1.0 / jnp.sum(expons, axis=1, keepdims=True))).astype(BF16)
        return carry

    lax.fori_loop(0, PATCHES // QB, soften, 0)

    arrived(g1.at[0 : T - 1], GA)
    total = g1[0]
    for i in range(1, T):
        total = total + g1[i]
    g2s[...] = total
    g2[pl.ds(x, 1)] = total.reshape(1, 1, D)

    arrived(vt.at[0:HEAD, 0 : PATCHES - ROWS], V)

    def send_g2(delta, carry):
        link(g2s, g2.at[x], GB, on_x(delta), tile).start()
        return carry

    lax.fori_loop(1, 8, send_g2, 0)
    arrived(gt.at[0:HEAD, 0 : PATCHES - ROWS], G)

    def backward(j, carry):
        at = pl.ds(pl.multiple_of(j * QB, QB), QB)
        grads = gt[:, at]
        dprobs = dot(grads.T, vt[...], 1, 0)
        low = probs[at, :]
        weight = low.astype(F32)
        prod = weight * dprobs
        spread = jnp.sum(prod, axis=1, keepdims=True)
        dscores = (prod - weight * spread).astype(BF16)
        dv[...] += dot(grads[0:HEAD], low, 1, 0)
        dk[...] += dot(qt[0:HEAD, at], dscores, 1, 0)
        dq = dot(kt[0:HEAD, :], dscores, 1, 1)
        dqb[:, at] = (dq * FACTOR).astype(BF16)
        return carry

    lax.fori_loop(0, PATCHES // QB, backward, 0)

    def columns(ref, t):
        return ref.at[:, pl.ds(pl.multiple_of(t * ROWS, ROWS), ROWS)]

    def back(src, dst, kind):
        dst[pl.ds(me80, HEAD), :] = src[:, pl.ds(me128, ROWS)]
        to_tiles(lambda t: link(columns(src, t), block_of(dst, tile), kind, img, t).start())

    dvb[...] = dv[...].astype(BF16)
    dkb[...] = (dk[...] * FACTOR).astype(BF16)
    back(dqb, bq, DQ)
    back(dvb, bv, DV)
    back(dkb, bk, DK)

    arrived(g2.at[0:7], GB)
    total = g2[0]
    for i in range(1, 8):
        total = total + g2[i]
    g3s[...] = total
    g3[pl.ds(z, 1)] = total.reshape(1, 1, D)

    def send_g3(delta, carry):
        link(g3s, g3.at[z], GC, on_z(delta), tile).start()
        return carry

    lax.fori_loop(1, 8, send_g3, 0)
    arrived(g3.at[0:7], GC)
    total = g3[0]
    for i in range(1, 8):
        total = total + g3[i]
    og_ref[...] = total

    for src, dst, kind in ((bq, oq_ref, DQ), (bv, ov_ref, DV), (bk, ok_ref, DK)):
        arrived(src.at[0 : D - HEAD], kind)
        for b in range(10):
            dst[:, b * 128 : (b + 1) * 128] = src[b * 128 : (b + 1) * 128, :].T

    sent(reqr.at[0 : T - 1], REQ)
    sent(wall.at[0, 0, 0:7], W1)
    sent(wall.at[0, 0:3], W2)
    sent(wall.at[0], W3)
    sent(rsend.at[0 : T - 1], ROW)
    for kind in (Q, K, V, G, DQ, DK, DV):
        sent(qs.at[0 : D - HEAD], kind)
    sent(g1.at[0 : T - 1], GA)
    sent(g2.at[0:7], GB)
    sent(g3.at[0:7], GC)


def body(query, keys, values, out_weight, hidden, gain, seq_grad, splice_at, merged_count):
    smem = pl.BlockSpec(memory_space=pltpu.SMEM)
    vmem = pl.BlockSpec(memory_space=pltpu.VMEM)
    block = jax.ShapeDtypeStruct((ROWS, D), BF16)
    head = pltpu.VMEM((128, PATCHES), BF16)
    blocks = pltpu.VMEM((D, ROWS), BF16)
    grads = pl.pallas_call(
        kernel,
        out_shape=(block, block, block, jax.ShapeDtypeStruct((1, D), F32)),
        in_specs=[smem, smem] + [vmem] * 7,
        out_specs=(vmem,) * 4,
        scratch_shapes=[
            *[blocks] * 4,
            *[head] * 4,
            pltpu.VMEM((2, 4, 8, 48, HALF), BF16),
            pltpu.VMEM((4, 1, 128), jnp.int32),
            pltpu.VMEM((T, 1, 128), jnp.int32),
            pltpu.VMEM((128, 128), F32),
            pltpu.VMEM((T, 32, HALF), BF16),
            pltpu.VMEM((T, 32, HALF), BF16),
            pltpu.VMEM((PATCHES, PATCHES), BF16),
            pltpu.VMEM((HEAD, PATCHES), F32),
            pltpu.VMEM((HEAD, PATCHES), F32),
            *[pltpu.VMEM((HEAD, PATCHES), BF16)] * 3,
            *[blocks] * 3,
            pltpu.VMEM((1, D), F32),
            pltpu.VMEM((T, 1, D), F32),
            pltpu.VMEM((1, D), F32),
            pltpu.VMEM((8, 1, D), F32),
            pltpu.VMEM((1, D), F32),
            pltpu.VMEM((8, 1, D), F32),
            pltpu.SemaphoreType.DMA((15,)),
            pltpu.SemaphoreType.DMA((15,)),
        ],
        compiler_params=pltpu.CompilerParams(
            collective_id=0, has_side_effects=True, vmem_limit_bytes=60 * 1024 * 1024
        ),
    )(
        splice_at,
        merged_count,
        query[0],
        keys[0],
        values[0],
        out_weight,
        hidden[0],
        gain[None, :],
        seq_grad[0],
    )
    return grads[0][None], grads[1][None], grads[2][None], grads[3][0]


def solution(mesh):
    rows = P("img", "tile", None)
    return jax.shard_map(
        body,
        mesh=mesh,
        in_specs=(rows, rows, rows, P("tile", None), rows, P(), rows, P("img", "tile"), P("img")),
        out_specs=(rows, rows, rows, P()),
        check_vma=False,
    )
```

```python
import math

import jax
import jax.numpy as jnp
from jax import lax
from jax.experimental import pallas as pl
from jax.experimental.pallas import tpu as pltpu
from jax.sharding import PartitionSpec as P

MESH = pl.DeviceIdType.MESH
F32 = jnp.float32
BF16 = jnp.bfloat16

NORM_EPS = 1e-06
HEAD = 80
D = 1280
T = 16
ROWS = 128
PATCHES = 2048
HALF = 640
QB = 256
FACTOR = HEAD ** (-0.5)
REQ, W1, W3, ROW, Q, K, V, DQ, DK, DV, GA, GB, GC, W2 = range(14)
G = W2 + 8


def dot(a, b, ca, cb):
    return lax.dot_general(a, b, (((ca,), (cb,)), ((), ())), preferred_element_type=F32)


def kernel(
    pos_ref, count_ref, gain_ref, q_hbm, k_hbm, v_hbm, w_hbm, h_hbm, seq_hbm,
    out_hbm, og_ref,
    q_ref, k_ref, v_ref, w_ref, h_ref, seq_ref,
    qs, ks, vs, gs, qt, kt, vt, gt, wall, reqs, reqr, reqt, rsend, rrecv,
    probs, dk, dqb, dkb, dvb, bq, bk, bv,
    g1s, g1, g2s, g2, g3s, g3, ssem, rsem, lsem,
):
    img = lax.axis_index("img")
    tile = lax.axis_index("tile")
    x, z = img // 8, img % 8
    y, c = tile // 2, tile % 2
    u = x * (1 - c) + z * c
    sigma = u // 2
    me80 = pl.multiple_of(tile * HEAD, 16)
    me128 = pl.multiple_of(tile * ROWS, ROWS)

    def peer(delta):
        return (tile + delta) % T

    def along(d):
        return ((x + (1 - c) * d) % 8) * 8 + (z + c * d) % 8

    def on_x(d):
        return ((x + d) % 8) * 8 + z

    def on_z(d):
        return x * 8 + (z + d) % 8

    def link(src, dst, kind, to_img, to_tile):
        return pltpu.make_async_remote_copy(
            src_ref=src,
            dst_ref=dst,
            send_sem=ssem.at[kind],
            recv_sem=rsem.at[kind],
            device_id=(to_img, to_tile),
            device_id_type=MESH,
        )

    def arrived(ref, kind):
        link(ref, ref, kind, img, peer(1)).wait_recv()

    def sent(ref, kind):
        link(ref, ref, kind, img, peer(1)).wait_send()

    def to_tiles(fn):
        def step(delta, carry):
            fn(peer(delta))
            return carry

        lax.fori_loop(1, T, step, 0)

    barrier = pltpu.get_barrier_semaphore()

    def hello(to_img, to_tile):
        pl.semaphore_signal(barrier, inc=1, device_id=(to_img, to_tile), device_id_type=MESH)

    def hello_plane(delta, carry):
        hello(on_x(delta), tile)
        hello(on_z(delta), tile)
        return carry

    to_tiles(lambda t: hello(img, t))
    lax.fori_loop(1, 8, hello_plane, 0)

    loads = [
        pltpu.make_async_copy(src, dst, lsem.at[i])
        for i, (src, dst) in enumerate(
            ((q_hbm, q_ref), (k_hbm, k_ref), (v_hbm, v_ref), (w_hbm, w_ref), (seq_hbm, seq_ref), (h_hbm, h_ref))
        )
    ]
    for load in loads:
        load.start()

    count = count_ref[...].reshape(1, 1)
    lane = lax.broadcasted_iota(jnp.int32, (8, 128), 1)
    span = lax.broadcasted_iota(jnp.int32, (8, 128), 0) * 4 + lane // 32
    slot = lane % 4
    part = (lane % 32) // 4
    seen = jnp.zeros((8, 128), jnp.int32)
    want = jnp.full((8, 128), -1, jnp.int32)
    whose = jnp.full((8, 128), -1, jnp.int32)
    for r in range(32):
        at = pos_ref[0, r]
        live = jnp.where(jnp.broadcast_to(count, (8, 128)) > tile * 32 + r, at // 128, -1)
        take = (span == live) & (seen == slot)
        want = jnp.where(take, at % 128, want)
        whose = jnp.where(take, r, whose)
        seen = seen + jnp.where(span == live, 1, 0)
    for o in range(4):
        reqs[o] = want[o : o + 1]

    row0 = lax.broadcasted_iota(jnp.int32, (48, PATCHES), 0) == 0
    key_at = lax.broadcasted_iota(jnp.int32, (48, PATCHES), 1)
    qt[HEAD:128, :] = jnp.where(row0, 1.0, 0.0).astype(BF16)
    kt[HEAD:128, :] = jnp.where(row0 & (key_at >= jnp.broadcast_to(4 * count, (48, PATCHES))), -1e30, 0.0).astype(BF16)
    vt[HEAD:128, :] = jnp.zeros((48, PATCHES), BF16)
    gt[HEAD:128, :] = jnp.zeros((48, PATCHES), BF16)
    dk[...] = jnp.zeros_like(dk)
    reqr[pl.ds(tile, 1)] = reqs[pl.ds(tile // 4, 1)]
    w_rows = pl.ds(pl.multiple_of((sigma // 2) * 32, 32), 48)
    w_cols = pl.ds(pl.multiple_of((sigma % 2) * HALF, 128), HALF)
    for i, (src, mid, dst) in enumerate(((q_ref, qs, qt), (k_ref, ks, kt), (v_ref, vs, vt))):
        loads[i].wait()
        for b in range(10):
            mid[b * 128 : (b + 1) * 128, :] = src[:, b * 128 : (b + 1) * 128].T
        dst[0:HEAD, pl.ds(me128, ROWS)] = mid[pl.ds(me80, HEAD), :]
    loads[3].wait()
    mine_too = (y + u) % 2 == 0

    @pl.when(mine_too)
    def _():
        wall[c, u, y // 2] = w_ref[w_rows, w_cols]

    pl.semaphore_wait(barrier, T - 1 + 14)

    to_tiles(lambda t: link(reqs.at[t // 4], reqr.at[tile], REQ, img, t).start())

    @pl.when(mine_too)
    def _():
        def send_w1(delta, carry):
            link(w_ref.at[w_rows, w_cols], wall.at[c, u, y // 2], W1, img, (tile + 2 * delta) % T).start()
            return carry

        lax.fori_loop(1, 8, send_w1, 0)

    arrived(reqr.at[0 : T - 1], REQ)
    loads[4].wait()
    asked = reqr[...].reshape(T, 128).astype(F32)
    reqt[...] = jnp.concatenate([asked, jnp.full((112, 128), -1.0, F32)], axis=0).T
    mine = reqt[pl.ds(pl.multiple_of((tile % 4) * 32, 32), 32), :].astype(jnp.int32)
    wide = lax.broadcasted_iota(jnp.int32, (32, 128), 1)
    row_part = lax.broadcasted_iota(jnp.int32, (32, 128), 0) // 4
    for d in range(0, T, 4):
        hits = [jnp.broadcast_to(mine[:, e : e + 1], (32, 128)) == wide for e in range(d, d + 4)]
        rows = jnp.zeros((128, HALF), F32)
        for s in range(8):
            pick = jnp.concatenate(
                [jnp.where(hit & (row_part == s), 1.0, 0.0) for hit in hits], axis=0
            ).astype(BF16)
            rows = rows + dot(pick, seq_ref[:, s * HALF : (s + 1) * HALF], 1, 0)
        rsend[d : d + 4] = rows.astype(BF16).reshape(4, 32, HALF)
    rrecv[pl.ds(tile, 1)] = rsend[pl.ds(tile, 1)]
    to_tiles(lambda t: link(rsend.at[t], rrecv.at[tile], ROW, img, t).start())

    def block_of(ref, t):
        return ref.at[pl.ds(pl.multiple_of(t * HEAD, 16), HEAD), :]

    def head_rows(ref):
        return ref.at[0:HEAD, pl.ds(me128, ROWS)]

    other = tile + 1 - 2 * c

    @pl.when(mine_too)
    def _():
        arrived(wall.at[0, 0, 0:3], W1)

    @pl.when((y + u) % 2 == 1)
    def _():
        arrived(wall.at[0, 0], W1)

    own = wall.at[c, u]
    link(own, own, W2 + 1, along(1), tile).start()
    link(own, own, W2 + 7, along(7), tile).start()
    link(own, own, W3, img, other).start()

    to_tiles(lambda t: link(block_of(qs, t), head_rows(qt), Q, img, t).start())

    def pass_on(d):
        arrived(wall.at[0, 0], W2 + d)
        more = wall.at[c, (u - d + 8) % 8]
        if d in (1, 2, 3):
            link(more, more, W2 + d + 1, along(1), tile).start()
        if d in (7, 6):
            link(more, more, W2 + d - 1, along(7), tile).start()
        link(more, more, W3, img, other).start()

    for d in (1, 7, 2, 6):
        pass_on(d)
    to_tiles(lambda t: link(block_of(ks, t), head_rows(kt), K, img, t).start())
    for d in (3, 5):
        pass_on(d)
    to_tiles(lambda t: link(block_of(vs, t), head_rows(vt), V, img, t).start())
    pass_on(4)

    loads[5].wait()
    hidden = h_ref[...].astype(F32)
    inverse = lax.rsqrt(jnp.mean(hidden * hidden, axis=1, keepdims=True) + NORM_EPS)
    normed = hidden * inverse
    wide_rows = lax.broadcasted_iota(jnp.int32, (ROWS, 128), 0)
    lane_part = (lax.broadcasted_iota(jnp.int32, (ROWS, 128), 1) % 32) // 4
    arrived(rrecv.at[0 : T - 1], ROW)
    halves = []
    for h in range(2):
        total = jnp.zeros((ROWS, HALF), F32)
        for o in range(4):
            owner = jnp.broadcast_to(whose[o : o + 1], (ROWS, 128))
            pick = (owner == wide_rows // 4) & (lane_part == 2 * (wide_rows % 4) + h)
            total = total + dot(
                jnp.where(pick, 1.0, 0.0).astype(BF16),
                rrecv[4 * o : 4 * o + 4].reshape(128, HALF),
                1,
                0,
            )
        halves.append(total)
    upstream = jnp.concatenate(halves, axis=1)
    both = upstream * normed
    part_sum = jnp.sum(both, axis=0, keepdims=True)
    gain = gain_ref[...].reshape(1, D)
    mean = jnp.mean(gain * both, axis=1, keepdims=True)
    attn = (inverse * (gain * upstream - normed * mean)).astype(BF16)
    g1s[...] = part_sum
    g1[pl.ds(tile, 1)] = part_sum.reshape(1, 1, D)

    arrived(wall.at[0], W3)
    for c2 in range(2):
        for ch in range(2):
            acc = jnp.zeros((384, ROWS), F32)
            for dh in range(2):
                acc = acc + dot(
                    wall[c2, 2 * (ch * 2 + dh) : 2 * (ch * 2 + dh) + 2].reshape(384, HALF), attn[:, dh * HALF : (dh + 1) * HALF], 1, 1
                )
            acc = acc.astype(BF16)
            for y2 in range(8):
                base = (2 * (2 * (y2 % 4) + y2 // 4) + c2) * HEAD
                if ch == 0:
                    gs[base : base + 48, :] = acc[48 * y2 : 48 * y2 + 48]
                else:
                    gs[base + 48 : base + 80, :] = acc[48 * y2 + 16 : 48 * y2 + 48]
    gt[0:HEAD, pl.ds(me128, ROWS)] = gs[pl.ds(me80, HEAD), :]
    to_tiles(lambda t: link(g1s, g1.at[tile], GA, img, t).start())

    def turn(i):
        return (8 + ((i + 1) // 2) * (2 * (i % 2) - 1)) % 8

    def send_g(i, carry):
        o = turn(i)
        for core in range(2):
            t = 2 * ((y + o) % 8) + core
            link(block_of(gs, t), head_rows(gt), G + (8 - o) % 8, img, t).start()
        return carry

    link(block_of(gs, other), head_rows(gt), G, img, other).start()
    lax.fori_loop(1, 8, send_g, 0)

    arrived(qt.at[0:HEAD, 0 : PATCHES - ROWS], Q)
    arrived(kt.at[0:HEAD, 0 : PATCHES - ROWS], K)
    rate = FACTOR * math.log2(math.e)

    def soften(j, carry):
        at = pl.ds(pl.multiple_of(j * QB, QB), QB)
        scores = dot(qt[:, at].T, kt[...], 1, 0)
        largest = jnp.max(scores, axis=1, keepdims=True)
        expons = jnp.exp2((scores - largest) * rate)
        probs[at, :] = (expons * (1.0 / jnp.sum(expons, axis=1, keepdims=True))).astype(BF16)
        return carry

    lax.fori_loop(0, PATCHES // QB, soften, 0)

    arrived(g1.at[0 : T - 1], GA)
    total = g1[0]
    for i in range(1, T):
        total = total + g1[i]
    g2s[...] = total
    g2[pl.ds(x, 1)] = total.reshape(1, 1, D)

    arrived(vt.at[0:HEAD, 0 : PATCHES - ROWS], V)

    def send_g2(delta, carry):
        link(g2s, g2.at[x], GB, on_x(delta), tile).start()
        return carry

    lax.fori_loop(1, 8, send_g2, 0)

    def columns(ref, t):
        return ref.at[:, pl.ds(pl.multiple_of(t * ROWS, ROWS), ROWS)]

    def back(src, dst, kind, t):
        link(columns(src, t), block_of(dst, tile), kind, img, t).start()

    def hand_back(src, dst, kind, i, j):
        @pl.when(i > 0)
        def _():
            back(src, dst, kind, 2 * j)
            back(src, dst, kind, 2 * j + 1)

        @pl.when(i == 0)
        def _():
            back(src, dst, kind, other)
            dst[pl.ds(me80, HEAD), :] = src[:, pl.ds(me128, ROWS)]

    def backward(i, carry):
        j = (y + turn(i)) % 8

        @pl.when(i == 0)
        def _():
            arrived(gt.at[0:HEAD, 0:ROWS], G)

        @pl.when(i > 0)
        def _():
            arrived(gt.at[0:HEAD, 0:QB], G + turn(i))

        at = pl.ds(pl.multiple_of(j * QB, QB), QB)
        dprobs = dot(gt[:, at].T, vt[...], 1, 0)
        weight = probs[at, :].astype(F32)
        prod = weight * dprobs
        spread = jnp.sum(prod, axis=1, keepdims=True)
        dscores = (prod - weight * spread).astype(BF16)
        dk[...] += dot(qt[0:HEAD, at], dscores, 1, 0)
        dq = dot(kt[0:HEAD, :], dscores, 1, 1)
        dqb[:, at] = (dq * FACTOR).astype(BF16)
        hand_back(dqb, bq, DQ, i, j)
        return carry

    lax.fori_loop(0, 8, backward, 0)
    dkb[...] = (dk[...] * FACTOR).astype(BF16)
    bk[pl.ds(me80, HEAD), :] = dkb[:, pl.ds(me128, ROWS)]
    to_tiles(lambda t: back(dkb, bk, DK, t))

    def value_grads(i, carry):
        j = (y + turn(i)) % 8
        at = pl.ds(pl.multiple_of(j * QB, QB), QB)
        dvb[:, at] = dot(gt[0:HEAD, :], probs[:, at], 1, 0).astype(BF16)
        hand_back(dvb, bv, DV, i, j)
        return carry

    lax.fori_loop(0, 8, value_grads, 0)

    arrived(g2.at[0:7], GB)
    total = g2[0]
    for i in range(1, 8):
        total = total + g2[i]
    g3s[...] = total
    g3[pl.ds(z, 1)] = total.reshape(1, 1, D)

    def send_g3(delta, carry):
        link(g3s, g3.at[z], GC, on_z(delta), tile).start()
        return carry

    lax.fori_loop(1, 8, send_g3, 0)
    arrived(g3.at[0:7], GC)
    total = g3[0]
    for i in range(1, 8):
        total = total + g3[i]
    og_ref[...] = total

    stores = []
    for i, (src, kind) in enumerate(((bq, DQ), (bk, DK), (bv, DV))):
        arrived(src.at[0 : D - HEAD], kind)
        stores.append(pltpu.make_async_copy(src, out_hbm.at[i], lsem.at[i]))
        stores[-1].start()
    for store in stores:
        store.wait()

    sent(reqr.at[0 : T - 1], REQ)

    @pl.when(mine_too)
    def _():
        sent(wall.at[0, 0:7, 0], W1)

    for d in range(1, 8):
        sent(wall.at[0, 0], W2 + d)
    sent(wall.at[0], W3)
    sent(rsend.at[0 : T - 1], ROW)
    for kind in (Q, K, V, DQ, DK, DV):
        sent(qs.at[0 : D - HEAD], kind)
    sent(qs.at[0:HEAD], G)
    for o in range(1, 8):
        sent(qs.at[0 : 2 * HEAD], G + o)
    sent(g1.at[0 : T - 1], GA)
    sent(g2.at[0:7], GB)
    sent(g3.at[0:7], GC)


def finish(in_hbm, g_ref, oq_hbm, ok_hbm, ov_hbm, og_ref, taken, turned, isem, osem):
    loads = [pltpu.make_async_copy(in_hbm.at[i], taken.at[i], isem.at[i]) for i in range(3)]
    for load in loads:
        load.start()
    og_ref[...] = g_ref[...].reshape(D)
    stores = []
    for i, out in enumerate((oq_hbm, ok_hbm, ov_hbm)):
        loads[i].wait()
        for b in range(10):
            turned[i, :, b * 128 : (b + 1) * 128] = taken[i, b * 128 : (b + 1) * 128, :].T
        stores.append(pltpu.make_async_copy(turned.at[i], out, osem.at[i]))
        stores[-1].start()
    for store in stores:
        store.wait()


def body(query, keys, values, out_weight, hidden, gain, seq_grad, splice_at, merged_count):
    smem = pl.BlockSpec(memory_space=pltpu.SMEM)
    vmem = pl.BlockSpec(memory_space=pltpu.VMEM)
    hbm = pl.BlockSpec(memory_space=pl.ANY)
    block = jax.ShapeDtypeStruct((ROWS, D), BF16)
    head = pltpu.VMEM((128, PATCHES), BF16)
    flat = pltpu.VMEM((ROWS, D), BF16)
    blocks = pltpu.VMEM((D, ROWS), BF16)
    grads, gain_grad = pl.pallas_call(
        kernel,
        out_shape=(jax.ShapeDtypeStruct((3, D, ROWS), BF16), jax.ShapeDtypeStruct((1, D), F32)),
        in_specs=[smem, vmem, vmem] + [hbm] * 6,
        out_specs=(hbm, vmem),
        scratch_shapes=[
            *[flat] * 3,
            pltpu.VMEM((HEAD, D), BF16),
            flat,
            pltpu.VMEM((ROWS, 4 * D), BF16),
            *[blocks] * 4,
            *[head] * 4,
            pltpu.VMEM((2, 8, 4, 48, HALF), BF16),
            pltpu.VMEM((4, 1, 128), jnp.int32),
            pltpu.VMEM((T, 1, 128), jnp.int32),
            pltpu.VMEM((128, 128), F32),
            pltpu.VMEM((T, 32, HALF), BF16),
            pltpu.VMEM((T, 32, HALF), BF16),
            pltpu.VMEM((PATCHES, PATCHES), BF16),
            pltpu.VMEM((HEAD, PATCHES), F32),
            *[pltpu.VMEM((HEAD, PATCHES), BF16)] * 3,
            *[blocks] * 3,
            pltpu.VMEM((1, D), F32),
            pltpu.VMEM((T, 1, D), F32),
            pltpu.VMEM((1, D), F32),
            pltpu.VMEM((8, 1, D), F32),
            pltpu.VMEM((1, D), F32),
            pltpu.VMEM((8, 1, D), F32),
            pltpu.SemaphoreType.DMA((29,)),
            pltpu.SemaphoreType.DMA((29,)),
            pltpu.SemaphoreType.DMA((6,)),
        ],
        compiler_params=pltpu.CompilerParams(
            collective_id=0, has_side_effects=True, vmem_limit_bytes=60 * 1024 * 1024
        ),
    )(
        splice_at,
        merged_count,
        gain,
        query[0],
        keys[0],
        values[0],
        out_weight,
        hidden[0],
        seq_grad[0],
    )
    oq, ok, ov, og = pl.pallas_call(
        finish,
        out_shape=(block, block, block, jax.ShapeDtypeStruct((D,), F32)),
        in_specs=[hbm, vmem],
        out_specs=(hbm, hbm, hbm, vmem),
        scratch_shapes=[
            pltpu.VMEM((3, D, ROWS), BF16),
            pltpu.VMEM((3, ROWS, D), BF16),
            pltpu.SemaphoreType.DMA((3,)),
            pltpu.SemaphoreType.DMA((3,)),
        ],
    )(grads, gain_grad)
    return oq[None], ok[None], ov[None], og


def solution(mesh):
    rows = P("img", "tile", None)
    return jax.shard_map(
        body,
        mesh=mesh,
        in_specs=(rows, rows, rows, P("tile", None), rows, P(), rows, P("img", "tile"), P("img")),
        out_specs=(rows, rows, rows, P()),
        check_vma=False,
    )
```
